32 devices in a mesh: ctx: 4 (over z), tp: 8 (over y, x, core).
Axes of the slice: x: 2, y: 2, z: 4, core: 2. Of those that a mesh axis runs over, the one named last changes fastest.
Arguments:
- query_states: bfloat16 [1024, 8192], P('ctx', 'tp'), may hold values from -6 to 6
- key_states: bfloat16 [1024, 1024], P('ctx'), may hold values from -6 to 6
- value_states: bfloat16 [1024, 1024], P('ctx'), may hold values from -6 to 6
- out_weight: bfloat16 [8192, 8192], P('tp'), may hold values from -0.5 to 0.5
- span_order: int32 [8], replicated, may hold values from 0 to 7, as said below
Outputs:
- projected: bfloat16 [1024, 8192], P('ctx', 'tp')
- z_loss: float32 [], replicated
The draws below stay inside these ranges and needn't reach their ends.
Inputs may be any that keep to these rules, and one draw needn't show every extreme that they name: span_order is a permutation of 0 to 7, and for every d the slots 2 d and 2 d + 1 hold spans c and 7 - c for some c.
All inputs are finite; a program needn't handle non-finite values.
Results may differ from the reference program's by a relative error of at most 0.0075.
Values may be sent and summed in bfloat16 or wider, within the bound.
A program may use at most 64 MiB of HBM per device.

```python
import math
import jax
import jax.numpy as jnp
from jax import lax

D = 8192
QH = 64
KVH = 8
HD = 128
SPAN = 128
SPANS = 8
TOKENS = 1024


def draw_key_states(key, part):
    values_drawn = jnp.clip(jax.random.normal(jax.random.fold_in(key, 11), (TOKENS, KVH * HD), jnp.float32), -6.0, 6.0)
    return values_drawn.astype(jnp.bfloat16)


def draw_query_states(key, part):
    values_drawn = jnp.clip(jax.random.normal(jax.random.fold_in(key, 12), (TOKENS, QH * HD), jnp.float32), -6.0, 6.0)
    return values_drawn.astype(jnp.bfloat16)


def draw_span_order(key, part):
    pair_count = SPANS // 2
    pair_ids = jax.random.permutation(jax.random.fold_in(key, 21), pair_count).astype(jnp.int32)
    flips = jax.random.randint(jax.random.fold_in(key, 22), (pair_count,), 0, 2)
    first = jnp.where(flips == 0, pair_ids, SPANS - 1 - pair_ids)
    second = SPANS - 1 - first
    return jnp.stack([first, second], axis=1).reshape(SPANS).astype(jnp.int32)


def level_of(rng, extent, shards, smallest, largest):
    def one(position, shards_of):
        steps = jax.random.uniform(jax.random.fold_in(jax.random.fold_in(rng, 6), position), (shards_of,), jnp.float32, smallest / len(shards), largest / len(shards))
        return jnp.repeat(jnp.exp(steps), extent[position] // shards_of).reshape((-1,) + (1,) * (len(extent) - position - 1))

    level = one(*shards[0])
    for cut in shards[1:]:
        level = level * one(*cut)
    return level


def normal_values(key, extent, deviation, reach, split=(), held_as=jnp.bfloat16):
    level = level_of(key, extent, split, -0.22, 0.18) if split else 1.0
    values = jax.random.normal(key, extent, jnp.float32) * deviation * level
    return jnp.minimum(jnp.maximum(values, -reach), reach).astype(held_as)


def setup_inputs(seed: int = 0) -> dict:
    streams_of = jax.random.split(jax.random.key(seed), 6)
    query_states = draw_query_states(jax.random.fold_in(streams_of[5], 71), 0)
    key_states = draw_key_states(jax.random.fold_in(streams_of[5], 71), 0)
    value_states = normal_values(streams_of[2], (TOKENS, KVH * HD), 1.0, 6.0, ((0, 4),))
    out_weight = normal_values(streams_of[3], (QH * HD, D), HD ** -0.5, 0.5, ((0, 8),))
    span_order = draw_span_order(jax.random.fold_in(streams_of[5], 71), 0)
    return dict(query_states=query_states, key_states=key_states, value_states=value_states, out_weight=out_weight, span_order=span_order)


z_coef = 0.01
neg_large = -1e+30

def reference(query_states, key_states, value_states, out_weight, span_order):
    group_size = QH // KVH
    slot_rows = jnp.arange(TOKENS, dtype=jnp.int32)
    positions = span_order[slot_rows // SPAN] * SPAN + slot_rows % SPAN
    visible = positions[None, :] <= positions[:, None]
    score_scale = 1.0 / math.sqrt(HD)

    def one_head(head_index):
        head_queries = lax.dynamic_slice_in_dim(query_states, (head_index * HD).astype(jnp.int32), HD, 1)
        kv_start = (head_index // group_size * HD).astype(jnp.int32)
        head_keys = lax.dynamic_slice_in_dim(key_states, kv_start, HD, 1)
        head_values = lax.dynamic_slice_in_dim(value_states, kv_start, HD, 1)
        scores = lax.dot_general(head_queries, head_keys, (((1,), (1,)), ((), ())), preferred_element_type=jnp.float32) * score_scale
        row_peak = lax.optimization_barrier(jnp.max(jnp.where(visible, scores, neg_large), axis=1))
        exp_terms = jnp.where(visible, jnp.exp(scores - row_peak[:, None]), 0.0)
        normalizer = lax.optimization_barrier(jnp.sum(exp_terms, axis=1))
        weights = exp_terms.astype(jnp.bfloat16)
        mixed = jnp.dot(weights, head_values, preferred_element_type=jnp.float32) / normalizer[:, None]
        return (mixed.astype(jnp.bfloat16), row_peak + jnp.log(normalizer))
    heads_out, log_norm = lax.map(one_head, jnp.arange(QH, dtype=jnp.int32))
    attended = jnp.transpose(heads_out, (1, 0, 2)).reshape(TOKENS, QH * HD)
    projected = jnp.dot(attended, out_weight, preferred_element_type=jnp.float32).astype(jnp.bfloat16)
    z_loss = z_coef * jnp.mean(log_norm * log_norm)
    return (projected, z_loss)
```

```python
import functools
import math

import jax
import jax.numpy as jnp
from jax import lax
from jax.experimental import pallas as pl
from jax.experimental.pallas import tpu as pltpu
from jax.sharding import PartitionSpec as P

QH = 64
KVH = 8
HD = 128

z_coef = 0.01
neg_large = -1e30
MESH = pl.DeviceIdType.MESH
LOG2E = math.log2(math.e)
LN2 = math.log(2.0)


def chunk_plan(chunk, tp):
    bits = tp.bit_length() - 1
    rest = list(range(1, bits))
    order = [0] + (rest if chunk % 2 == 0 else rest[::-1])
    kept = list(range(tp))
    slots, sends, keeps = {}, [], []
    offset = 0
    for stage, bit in enumerate(order):
        send = [e for e in kept if (e >> bit) & 1]
        kept = [e for e in kept if not (e >> bit) & 1]
        for e in kept:
            slots[stage, e] = offset
            offset += 1
        sends.append(send)
        keeps.append(list(kept))
    return order, slots, sends, keeps


def kernel(
    n_ctx, tp, heads, chunks, count,
    so_ref, q_hbm, k_hbm, v_hbm, w_hbm, out_ref, z_ref,
    qbuf, kbuf, vbuf, wbuf, bias, att, acc, sbuf, rbuf, zctx, zsend, zrecv,
    local_sem, w_sem, kv_send, kv_recv, rs_send, rs_recv, zc_send, zc_recv, zt_send, zt_recv,
):
    z = lax.axis_index("ctx")
    t = lax.axis_index("tp")
    bits = tp.bit_length() - 1
    rows = qbuf.shape[0]
    span_rows = rows // 2
    width = wbuf.shape[-1]
    cols = width * chunks
    tbit = [lax.rem(lax.div(t, 1 << b), 2) for b in range(bits)]

    def owner(e):
        d = 0
        for b in range(bits):
            d = d + ((1 - tbit[b]) if (e >> b) & 1 else tbit[b]) * (1 << b)
        return d

    def partner(bit):
        return t + (1 - 2 * tbit[bit]) * (1 << bit)

    plans = [chunk_plan(c, tp) for c in range(chunks)]

    kv_start = pl.multiple_of(lax.div(t * heads, QH // KVH) * HD, HD)
    own = pl.ds(pl.multiple_of(z * rows, rows), rows)
    k_in = pltpu.make_async_copy(k_hbm.at[:, pl.ds(kv_start, HD)], kbuf.at[own, :], local_sem.at[0])
    v_in = pltpu.make_async_copy(v_hbm.at[:, pl.ds(kv_start, HD)], vbuf.at[own, :], local_sem.at[1])
    q_in = pltpu.make_async_copy(q_hbm, qbuf, local_sem.at[2])
    k_in.start()
    v_in.start()
    q_in.start()

    barrier = pltpu.get_barrier_semaphore()
    for r in range(1, n_ctx):
        pl.semaphore_signal(barrier, inc=1, device_id=(lax.rem(z + r, n_ctx), t), device_id_type=MESH)
    for b in range(bits):
        pl.semaphore_signal(barrier, inc=1, device_id=(z, partner(b)), device_id_type=MESH)

    w_in = {}
    for c in range(chunks):
        _, _, sends, keeps = plans[c]
        for e in sends[0] + keeps[0]:
            start = pl.multiple_of(owner(e) * cols + c * width, width)
            w_in[c, e] = pltpu.make_async_copy(
                w_hbm.at[:, pl.ds(start, width)], wbuf.at[c, e], w_sem.at[c, e]
            )
            w_in[c, e].start()
    pl.semaphore_wait(barrier, n_ctx - 1 + bits)

    def piece(which, j):
        return (kbuf, vbuf)[which].at[pl.ds(pl.multiple_of(j * rows, rows), rows), :]

    def kv_copy(d, dist, which):
        step = 1 - 2 * d
        ref = piece(which, z - step * dist)
        return pltpu.make_async_remote_copy(
            src_ref=ref, dst_ref=ref,
            send_sem=kv_send.at[d, dist, which], recv_sem=kv_recv.at[d, dist, which],
            device_id=(z + step, t), device_id_type=MESH,
        )

    def kv_arrival(d, dist, which):
        step = 1 - 2 * d
        ref = piece(which, z - step * dist)
        return pltpu.make_async_remote_copy(
            src_ref=ref, dst_ref=ref,
            send_sem=kv_send.at[d, dist - 1, which], recv_sem=kv_recv.at[d, dist - 1, which],
            device_id=(z + step, t), device_id_type=MESH,
        )

    def can_send(d, dist):
        if d == 0:
            return jnp.logical_and(z >= dist, z + 1 < n_ctx)
        return jnp.logical_and(z + dist < n_ctx, z >= 1)

    def has_source(d, dist):
        return z >= dist if d == 0 else z + dist < n_ctx

    for which in range(2):
        (k_in, v_in)[which].wait()
        for d in range(2):
            @pl.when(can_send(d, 0))
            def _(d=d, which=which):
                kv_copy(d, 0, which).start()

    for half in range(2):
        q_pos = so_ref[2 * z + half] * span_rows + lax.broadcasted_iota(jnp.int32, (span_rows, span_rows), 0)
        for s in range(2 * n_ctx):
            k_pos = so_ref[s] * span_rows + lax.broadcasted_iota(jnp.int32, (span_rows, span_rows), 1)
            bias[half * span_rows:(half + 1) * span_rows, s * span_rows:(s + 1) * span_rows] = jnp.where(
                k_pos <= q_pos, 0.0, neg_large
            )
    q_in.wait()

    for dist in range(1, n_ctx):
        for which in range(2):
            for d in range(2):
                @pl.when(has_source(d, dist))
                def _(d=d, which=which, dist=dist):
                    kv_arrival(d, dist, which).wait_recv()

                @pl.when(can_send(d, dist))
                def _(d=d, which=which, dist=dist):
                    kv_copy(d, dist, which).start()

    def one_head(h, squares):
        lanes = pl.ds(pl.multiple_of(h * HD, HD), HD)
        scores = lax.dot_general(
            qbuf[:, lanes], kbuf[...], (((1,), (1,)), ((), ())), preferred_element_type=jnp.float32
        ) * (LOG2E / math.sqrt(HD)) + bias[...]
        peak = jnp.max(scores, axis=1, keepdims=True)
        terms = jnp.exp2(scores - peak)
        normalizer = jnp.sum(terms, axis=1, keepdims=True)
        weighted = jnp.dot(terms.astype(jnp.bfloat16), vbuf[...], preferred_element_type=jnp.float32)
        att[:, lanes] = (weighted / normalizer).astype(jnp.bfloat16)
        log_norm = peak * LN2 + jnp.log(normalizer)
        return squares + log_norm * log_norm

    squares = lax.fori_loop(0, heads, one_head, jnp.zeros((rows, 1), jnp.float32))
    zctx[0] = jnp.broadcast_to(jnp.sum(squares, axis=0, keepdims=True), zctx.shape[1:])

    def zc_copy(r):
        return pltpu.make_async_remote_copy(
            src_ref=zctx.at[0], dst_ref=zctx.at[r], send_sem=zc_send.at[r], recv_sem=zc_recv.at[r],
            device_id=(lax.rem(z + r, n_ctx), t), device_id_type=MESH,
        )

    for r in range(1, n_ctx):
        zc_copy(r).start()

    def rs_copy(c, stage, e_kept):
        order, slots, _, _ = plans[c]
        slot = slots[stage, e_kept]
        return pltpu.make_async_remote_copy(
            src_ref=sbuf.at[c, slot], dst_ref=rbuf.at[c, slot],
            send_sem=rs_send.at[c, slot], recv_sem=rs_recv.at[c, slot],
            device_id=(z, partner(order[stage])), device_id_type=MESH,
        )

    def push(c, stage, e, value):
        order, slots, _, _ = plans[c]
        e_kept = e ^ (1 << order[stage])
        sbuf[c, slots[stage, e_kept]] = value.astype(jnp.bfloat16)
        rs_copy(c, stage, e_kept).start()

    def project(c):
        _, slots, sends, keeps = plans[c]
        for e in sends[0]:
            w_in[c, e].wait()
            push(c, 0, e, jnp.dot(att[...], wbuf[c, e], preferred_element_type=jnp.float32))
        for e in keeps[0]:
            w_in[c, e].wait()
            acc[c, slots[0, e]] = jnp.dot(att[...], wbuf[c, e], preferred_element_type=jnp.float32)

    def combine(c, stage):
        order, slots, sends, keeps = plans[c]
        later = sends[stage + 1] + keeps[stage + 1] if stage + 1 < bits else [0]
        for e in later:
            rs_copy(c, stage, e).wait_recv()
            value = acc[c, slots[0, e]] + rbuf[c, slots[stage, e]].astype(jnp.float32)
            if stage + 1 == bits:
                out_ref[:, c * width:(c + 1) * width] = value.astype(jnp.bfloat16)
            elif e in sends[stage + 1]:
                push(c, stage + 1, e, value)
            else:
                acc[c, slots[0, e]] = value

    for c in range(chunks):
        project(c)
        if c >= 1:
            combine(c - 1, 0)
    combine(chunks - 1, 0)

    for r in range(1, n_ctx):
        zc_copy(r).wait_recv()
    total = zctx[lax.rem(z, n_ctx)]
    for j in range(1, n_ctx):
        total = total + zctx[lax.rem(z - j + n_ctx, n_ctx)]

    def zt_copy(b):
        return pltpu.make_async_remote_copy(
            src_ref=zsend.at[b], dst_ref=zrecv.at[b], send_sem=zt_send.at[b], recv_sem=zt_recv.at[b],
            device_id=(z, partner(b)), device_id_type=MESH,
        )

    for b in range(bits):
        zsend[b] = total
        zt_copy(b).start()
        if b + 1 < bits:
            for c in range(chunks):
                combine(c, b + 1)
        zt_copy(b).wait_recv()
        total = total + zrecv[b]
    z_ref[...] = total[0:1, 0:1] * (z_coef / count)

    for which in range(2):
        for d in range(2):
            for dist in range(n_ctx - 1):
                @pl.when(can_send(d, dist))
                def _(d=d, which=which, dist=dist):
                    kv_copy(d, dist, which).wait_send()
    for r in range(1, n_ctx):
        zc_copy(r).wait_send()
    for b in range(bits):
        zt_copy(b).wait_send()
    for c in range(chunks):
        order, slots, _, keeps = plans[c]
        for stage in range(bits):
            for e in keeps[stage]:
                rs_copy(c, stage, e).wait_send()


def on_device(n_ctx, tp, query_states, key_states, value_states, out_weight, span_order):
    rows, q_cols = query_states.shape
    heads = q_cols // HD
    depth, model = out_weight.shape
    cols = model // tp
    width = min(256, cols)
    chunks = cols // width
    bits = tp.bit_length() - 1
    tokens = rows * n_ctx
    any_spec = pl.BlockSpec(memory_space=pl.ANY)
    vmem_spec = pl.BlockSpec(memory_space=pltpu.VMEM)
    dma = pltpu.SemaphoreType.DMA
    projected, z_loss = pl.pallas_call(
        functools.partial(kernel, n_ctx, tp, heads, chunks, QH * tokens),
        out_shape=(
            jax.ShapeDtypeStruct((rows, cols), jnp.bfloat16),
            jax.ShapeDtypeStruct((1, 1), jnp.float32),
        ),
        in_specs=[pl.BlockSpec(memory_space=pltpu.SMEM)] + [any_spec] * 4,
        out_specs=(vmem_spec, vmem_spec),
        scratch_shapes=[
            pltpu.VMEM((rows, q_cols), jnp.bfloat16),
            pltpu.VMEM((tokens, HD), jnp.bfloat16),
            pltpu.VMEM((tokens, HD), jnp.bfloat16),
            pltpu.VMEM((chunks, tp, depth, width), jnp.bfloat16),
            pltpu.VMEM((rows, tokens), jnp.float32),
            pltpu.VMEM((rows, q_cols), jnp.bfloat16),
            pltpu.VMEM((chunks, tp // 2, rows, width), jnp.float32),
            pltpu.VMEM((chunks, tp - 1, rows, width), jnp.bfloat16),
            pltpu.VMEM((chunks, tp - 1, rows, width), jnp.bfloat16),
            pltpu.VMEM((n_ctx, 8, 128), jnp.float32),
            pltpu.VMEM((bits, 8, 128), jnp.float32),
            pltpu.VMEM((bits, 8, 128), jnp.float32),
            dma((3,)),
            dma((chunks, tp)),
            dma((2, n_ctx, 2)),
            dma((2, n_ctx, 2)),
            dma((chunks, tp - 1)),
            dma((chunks, tp - 1)),
            dma((n_ctx,)),
            dma((n_ctx,)),
            dma((bits,)),
            dma((bits,)),
        ],
        compiler_params=pltpu.CompilerParams(collective_id=0, has_side_effects=True),
    )(span_order, query_states, key_states, value_states, out_weight)
    return projected, z_loss.reshape(())


def solution(mesh):
    return jax.shard_map(
        functools.partial(on_device, mesh.shape["ctx"], mesh.shape["tp"]),
        mesh=mesh,
        in_specs=(P("ctx", "tp"), P("ctx", None), P("ctx", None), P("tp", None), P()),
        out_specs=(P("ctx", "tp"), P()),
        check_vma=False,
    )
```

```python
import functools
import math

import jax
import jax.numpy as jnp
from jax import lax
from jax.experimental import pallas as pl
from jax.experimental.pallas import tpu as pltpu
from jax.sharding import PartitionSpec as P

QH = 64
KVH = 8
HD = 128

z_coef = 0.01
neg_large = -1e30
MESH = pl.DeviceIdType.MESH
LOG2E = math.log2(math.e)
LN2 = math.log(2.0)


def chunk_plan(chunk, tp):
    bits = tp.bit_length() - 1
    rest = list(range(1, bits))
    order = [0] + (rest if chunk % 2 == 0 else rest[::-1])
    kept = list(range(tp))
    slots, sends, keeps = {}, [], []
    offset = 0
    for stage, bit in enumerate(order):
        send = [e for e in kept if (e >> bit) & 1]
        kept = [e for e in kept if not (e >> bit) & 1]
        for e in kept:
            slots[stage, e] = offset
            offset += 1
        sends.append(send)
        keeps.append(list(kept))
    return order, slots, sends, keeps


def kernel(
    n_ctx, tp, heads, chunks, count,
    so_ref, q_hbm, k_hbm, v_hbm, w_hbm, out_ref, z_ref,
    qbuf, kbuf, vbuf, wbuf, bias, att, acc, sbuf, rbuf, zctx, zsend, zrecv,
    local_sem, w_sem, kv_send, kv_recv, rs_send, rs_recv, zc_send, zc_recv, zt_send, zt_recv,
):
    z = lax.axis_index("ctx")
    t = lax.axis_index("tp")
    bits = tp.bit_length() - 1
    rows = qbuf.shape[0]
    span_rows = rows // 2
    width = sbuf.shape[-1]
    cols = width * chunks
    tbit = [lax.rem(lax.div(t, 1 << b), 2) for b in range(bits)]

    def owner(e):
        d = 0
        for b in range(bits):
            d = d + ((1 - tbit[b]) if (e >> b) & 1 else tbit[b]) * (1 << b)
        return d

    def partner(bit):
        return t + (1 - 2 * tbit[bit]) * (1 << bit)

    plans = [chunk_plan(c, tp) for c in range(chunks)]

    kv_start = pl.multiple_of(lax.div(t * heads, QH // KVH) * HD, HD)
    own = pl.ds(pl.multiple_of(z * rows, rows), rows)
    k_in = pltpu.make_async_copy(k_hbm.at[:, pl.ds(kv_start, HD)], kbuf.at[own, :], local_sem.at[0])
    v_in = pltpu.make_async_copy(v_hbm.at[:, pl.ds(kv_start, HD)], vbuf.at[own, :], local_sem.at[1])
    q_in = pltpu.make_async_copy(q_hbm, qbuf, local_sem.at[2])
    k_in.start()
    v_in.start()
    q_in.start()

    barrier = pltpu.get_barrier_semaphore()
    for r in range(1, n_ctx):
        pl.semaphore_signal(barrier, inc=1, device_id=(lax.rem(z + r, n_ctx), t), device_id_type=MESH)
    for b in range(bits):
        pl.semaphore_signal(barrier, inc=1, device_id=(z, partner(b)), device_id_type=MESH)

    w_in = {}
    for c in range(chunks):
        _, _, sends, keeps = plans[c]
        for place, e in enumerate(sends[0] + keeps[0]):
            start = pl.multiple_of(owner(e) * cols + c * width, width)
            w_in[c, e] = pltpu.make_async_copy(
                w_hbm.at[:, pl.ds(start, width)],
                wbuf.at[c, :, pl.ds(place * width, width)],
                w_sem.at[c, e],
            )
            w_in[c, e].start()
    pl.semaphore_wait(barrier, n_ctx - 1 + bits)

    def piece(which, j):
        return (kbuf, vbuf)[which].at[pl.ds(pl.multiple_of(j * rows, rows), rows), :]

    def kv_copy(d, dist, which):
        step = 1 - 2 * d
        ref = piece(which, z - step * dist)
        return pltpu.make_async_remote_copy(
            src_ref=ref, dst_ref=ref,
            send_sem=kv_send.at[d, dist, which], recv_sem=kv_recv.at[d, dist, which],
            device_id=(z + step, t), device_id_type=MESH,
        )

    def kv_arrival(d, dist, which):
        step = 1 - 2 * d
        ref = piece(which, z - step * dist)
        return pltpu.make_async_remote_copy(
            src_ref=ref, dst_ref=ref,
            send_sem=kv_send.at[d, dist - 1, which], recv_sem=kv_recv.at[d, dist - 1, which],
            device_id=(z + step, t), device_id_type=MESH,
        )

    def can_send(d, dist):
        if d == 0:
            return jnp.logical_and(z >= dist, z + 1 < n_ctx)
        return jnp.logical_and(z + dist < n_ctx, z >= 1)

    def has_source(d, dist):
        return z >= dist if d == 0 else z + dist < n_ctx

    for which in range(2):
        (k_in, v_in)[which].wait()
        for d in range(2):
            @pl.when(can_send(d, 0))
            def _(d=d, which=which):
                kv_copy(d, 0, which).start()

    for half in range(2):
        q_pos = so_ref[2 * z + half] * span_rows + lax.broadcasted_iota(jnp.int32, (span_rows, span_rows), 0)
        for s in range(2 * n_ctx):
            k_pos = so_ref[s] * span_rows + lax.broadcasted_iota(jnp.int32, (span_rows, span_rows), 1)
            bias[half * span_rows:(half + 1) * span_rows, s * span_rows:(s + 1) * span_rows] = jnp.where(
                k_pos <= q_pos, 0.0, neg_large
            )
    q_in.wait()
    for dist in range(1, n_ctx):
        for which in range(2):
            for d in range(2):
                @pl.when(has_source(d, dist))
                def _(d=d, which=which, dist=dist):
                    kv_arrival(d, dist, which).wait_recv()

                @pl.when(can_send(d, dist))
                def _(d=d, which=which, dist=dist):
                    kv_copy(d, dist, which).start()

    def one_head(h, squares):
        lanes = pl.ds(pl.multiple_of(h * HD, HD), HD)
        scores = lax.dot_general(
            qbuf[:, lanes], kbuf[...], (((1,), (1,)), ((), ())), preferred_element_type=jnp.float32
        ) * (LOG2E / math.sqrt(HD)) + bias[...]
        peak = jnp.max(scores, axis=1, keepdims=True)
        terms = jnp.exp2(scores - peak)
        normalizer = jnp.sum(terms, axis=1, keepdims=True)
        weighted = jnp.dot(terms.astype(jnp.bfloat16), vbuf[...], preferred_element_type=jnp.float32)
        att[:, lanes] = (weighted / normalizer).astype(jnp.bfloat16)
        log_norm = peak * LN2 + jnp.log(normalizer)
        return squares + log_norm * log_norm

    squares = lax.fori_loop(0, heads, one_head, jnp.zeros((rows, 1), jnp.float32))
    zctx[0] = jnp.broadcast_to(jnp.sum(squares, axis=0, keepdims=True), zctx.shape[1:])

    def zc_copy(r):
        return pltpu.make_async_remote_copy(
            src_ref=zctx.at[0], dst_ref=zctx.at[r], send_sem=zc_send.at[r], recv_sem=zc_recv.at[r],
            device_id=(lax.rem(z + r, n_ctx), t), device_id_type=MESH,
        )

    for r in range(1, n_ctx):
        zc_copy(r).start()

    def rs_copy(c, stage, e_kept):
        order, slots, _, _ = plans[c]
        slot = slots[stage, e_kept]
        return pltpu.make_async_remote_copy(
            src_ref=sbuf.at[c, slot], dst_ref=rbuf.at[c, slot],
            send_sem=rs_send.at[c, slot], recv_sem=rs_recv.at[c, slot],
            device_id=(z, partner(order[stage])), device_id_type=MESH,
        )

    def push(c, stage, e, value):
        order, slots, _, _ = plans[c]
        e_kept = e ^ (1 << order[stage])
        sbuf[c, slots[stage, e_kept]] = value.astype(jnp.bfloat16)
        rs_copy(c, stage, e_kept).start()

    def project(c):
        _, slots, sends, keeps = plans[c]
        for group, blocks in enumerate((sends[0], keeps[0])):
            for e in blocks:
                w_in[c, e].wait()
            span = len(blocks) * width
            products = jnp.dot(
                att[...], wbuf[c, :, group * span:(group + 1) * span], preferred_element_type=jnp.float32
            )
            for place, e in enumerate(blocks):
                value = products[:, place * width:(place + 1) * width]
                if group == 0:
                    push(c, 0, e, value)
                else:
                    acc[c, slots[0, e]] = value

    def combine(c, stage):
        order, slots, sends, keeps = plans[c]
        later = sends[stage + 1] + keeps[stage + 1] if stage + 1 < bits else [0]
        for e in later:
            rs_copy(c, stage, e).wait_recv()
            value = acc[c, slots[0, e]] + rbuf[c, slots[stage, e]].astype(jnp.float32)
            if stage + 1 == bits:
                out_ref[:, c * width:(c + 1) * width] = value.astype(jnp.bfloat16)
            elif e in sends[stage + 1]:
                push(c, stage + 1, e, value)
            else:
                acc[c, slots[0, e]] = value

    def zt_copy(b):
        return pltpu.make_async_remote_copy(
            src_ref=zsend.at[b], dst_ref=zrecv.at[b], send_sem=zt_send.at[b], recv_sem=zt_recv.at[b],
            device_id=(z, partner(b)), device_id_type=MESH,
        )

    def z_steps():
        for r in range(1, n_ctx):
            zc_copy(r).wait_recv()
        total = zctx[z]
        for j in range(1, n_ctx):
            total = total + zctx[lax.rem(z - j + n_ctx, n_ctx)]
        for b in range(bits):
            zsend[b] = total
            zt_copy(b).start()
            yield
            zt_copy(b).wait_recv()
            total = total + zrecv[b]
        z_ref[...] = total[0:1, 0:1] * (z_coef / count)
        yield

    z_next = z_steps()
    for c in range(chunks):
        project(c)
        if c >= 1:
            combine(c - 1, 0)
            next(z_next, None)
    combine(chunks - 1, 0)
    for stage in range(1, bits):
        for c in range(chunks):
            combine(c, stage)
            next(z_next, None)
    for _ in z_next:
        pass

    for which in range(2):
        for d in range(2):
            for dist in range(n_ctx - 1):
                @pl.when(can_send(d, dist))
                def _(d=d, which=which, dist=dist):
                    kv_copy(d, dist, which).wait_send()
    for r in range(1, n_ctx):
        zc_copy(r).wait_send()
    for b in range(bits):
        zt_copy(b).wait_send()
    for c in range(chunks):
        order, slots, _, keeps = plans[c]
        for stage in range(bits):
            for e in keeps[stage]:
                rs_copy(c, stage, e).wait_send()


def on_device(n_ctx, tp, query_states, key_states, value_states, out_weight, span_order):
    rows, q_cols = query_states.shape
    heads = q_cols // HD
    depth, model = out_weight.shape
    cols = model // tp
    width = min(256, cols)
    chunks = cols // width
    bits = tp.bit_length() - 1
    tokens = rows * n_ctx
    any_spec = pl.BlockSpec(memory_space=pl.ANY)
    vmem_spec = pl.BlockSpec(memory_space=pltpu.VMEM)
    dma = pltpu.SemaphoreType.DMA
    projected, z_loss = pl.pallas_call(
        functools.partial(kernel, n_ctx, tp, heads, chunks, QH * tokens),
        out_shape=(
            jax.ShapeDtypeStruct((rows, cols), jnp.bfloat16),
            jax.ShapeDtypeStruct((1, 1), jnp.float32),
        ),
        in_specs=[pl.BlockSpec(memory_space=pltpu.SMEM)] + [any_spec] * 4,
        out_specs=(vmem_spec, vmem_spec),
        scratch_shapes=[
            pltpu.VMEM((rows, q_cols), jnp.bfloat16),
            pltpu.VMEM((tokens, HD), jnp.bfloat16),
            pltpu.VMEM((tokens, HD), jnp.bfloat16),
            pltpu.VMEM((chunks, depth, tp * width), jnp.bfloat16),
            pltpu.VMEM((rows, tokens), jnp.float32),
            pltpu.VMEM((rows, q_cols), jnp.bfloat16),
            pltpu.VMEM((chunks, tp // 2, rows, width), jnp.float32),
            pltpu.VMEM((chunks, tp - 1, rows, width), jnp.bfloat16),
            pltpu.VMEM((chunks, tp - 1, rows, width), jnp.bfloat16),
            pltpu.VMEM((n_ctx, 8, 128), jnp.float32),
            pltpu.VMEM((bits, 8, 128), jnp.float32),
            pltpu.VMEM((bits, 8, 128), jnp.float32),
            dma((3,)),
            dma((chunks, tp)),
            dma((2, n_ctx, 2)),
            dma((2, n_ctx, 2)),
            dma((chunks, tp - 1)),
            dma((chunks, tp - 1)),
            dma((n_ctx,)),
            dma((n_ctx,)),
            dma((bits,)),
            dma((bits,)),
        ],
        compiler_params=pltpu.CompilerParams(collective_id=0, has_side_effects=True),
    )(span_order, query_states, key_states, value_states, out_weight)
    return projected, z_loss.reshape(())


def solution(mesh):
    return jax.shard_map(
        functools.partial(on_device, mesh.shape["ctx"], mesh.shape["tp"]),
        mesh=mesh,
        in_specs=(P("ctx", "tp"), P("ctx", None), P("ctx", None), P("tp", None), P()),
        out_specs=(P("ctx", "tp"), P()),
        check_vma=False,
    )
```
